256 devices in a mesh: rows: 32 (over x, z), grp: 8 (over y, core).
Axes of the slice: x: 4, y: 4, z: 8, core: 2. Of those that a mesh axis runs over, the one named last changes fastest.
Arguments:
- embeddings: bfloat16 [131072, 1024], P(('rows', 'grp')), may hold values from -6 to 6
- coarse_ids: int32 [131072], P(('rows', 'grp')), may hold values from 0 to 2047, as said below
- fine_ids: int32 [131072], P(('rows', 'grp')), may hold values from 0 to 63, as said below
- coarse_old: float32 [2048, 1024], P(('rows', 'grp')), may hold values from -6 to 6
- fine_old: float32 [2048, 64, 1024], P('rows', 'grp'), may hold values from -6 to 6
Outputs:
- coarse_new: float32 [2048, 1024], P(('rows', 'grp'))
- fine_new: float32 [2048, 64, 1024], P('rows', 'grp')
- distances: float32 [131072], P(('rows', 'grp'))
The draws below stay inside these ranges and needn't reach their ends.
Inputs may be any that keep to these rules, and one draw needn't show every extreme that they name: Among the 512 rows of one device, at most 4 have the same pair (coarse_ids // 64, fine_ids // 8), and in every such block some pair has exactly 4. `fine_ids`: within each coarse cluster's fine centroids.
All inputs are finite; a program needn't handle non-finite values.
Results may differ from the reference program's by a relative error of at most 0.0003.
Values may be sent and summed in bfloat16 or wider, within the bound.
No kernel may reach another device: no remote copies, remote signals or barrier semaphores. Data moves between devices by JAX's collectives and lax.ppermute only.
A program may use at most 64 MiB of HBM per device.

```python
import jax
import jax.numpy as jnp

D = 1024
K = 2048
F = 64
ROWS_DEV = 512
SLOTS = 4
KC = 64
FG = 8
TOTAL_ROWS = 131072
N_GRP = 8
DEVICES = 256


def route_ids(key):
    dests = DEVICES
    total_slots = dests * SLOTS

    def one_block(block_key):
        parts = jax.random.split(block_key, 6)
        hotness = (jax.random.randint(parts[0], (dests,), 0, 4) == 0).astype(jnp.int32)
        first_dest = jax.random.randint(parts[1], (), 0, dests)
        slot_index = jnp.arange(total_slots, dtype=jnp.int32)
        owner_of = slot_index // SLOTS
        priority = jax.random.randint(parts[2], (total_slots,), 0, 2 ** 15)
        priority = priority - hotness[owner_of] * 2 ** 14 - (owner_of == first_dest).astype(jnp.int32) * 2 ** 16
        scores = priority * 8192 + slot_index
        chosen = jnp.argsort(scores, stable=True)[:ROWS_DEV]
        chosen = jax.random.permutation(parts[3], chosen)
        target = chosen // SLOTS
        coarse = target // N_GRP * KC + jax.random.randint(parts[4], (ROWS_DEV,), 0, KC)
        fine = target % N_GRP * FG + jax.random.randint(parts[5], (ROWS_DEV,), 0, FG)
        return (coarse.astype(jnp.int32), fine.astype(jnp.int32))
    block_keys = jax.random.split(jax.random.fold_in(key, 7), DEVICES)
    coarse, fine = jax.vmap(one_block)(block_keys)
    return (coarse.reshape(-1), fine.reshape(-1))


def draw_coarse_ids(key, part):
    return route_ids(key)[0]


def draw_fine_ids(key, part):
    return route_ids(key)[1]


def block_scale(stream_key, extent, cuts, smallest, high):
    gain, own = 1.0, jax.random.fold_in(stream_key, 6)
    for axis_at, blocks in cuts:
        steps = jnp.exp(jax.random.uniform(jax.random.fold_in(own, axis_at), (blocks,), jnp.float32, smallest / len(cuts), high / len(cuts)))
        gain = gain * jnp.repeat(steps, extent[axis_at] // blocks).reshape([-1 if axis == axis_at else 1 for axis in range(len(extent))])
    return gain


def normal_values(own_key, shape, scale, reach, cuts=(), kind=jnp.bfloat16):
    factor_of = block_scale(own_key, shape, cuts, -0.22, 0.18) if cuts else 1.0
    result = jax.random.normal(own_key, shape, jnp.float32) * scale * factor_of
    return jnp.minimum(jnp.maximum(result, -reach), reach).astype(kind)


def setup_inputs(seed: int = 0) -> dict:
    seeds = jax.random.split(jax.random.key(seed), 6)
    return {
        "embeddings": normal_values(seeds[0], (TOTAL_ROWS, D), 1.0, 6.0, ((0, 256),)),
        "coarse_ids": draw_coarse_ids(jax.random.fold_in(seeds[5], 71), 0),
        "fine_ids": draw_fine_ids(jax.random.fold_in(seeds[5], 71), 0),
        "coarse_old": normal_values(seeds[3], (K, D), 1.0, 6.0, ((0, 256),), jnp.float32),
        "fine_old": normal_values(seeds[4], (K, F, D), 1.0, 6.0, ((0, 32), (1, 8)), jnp.float32),
    }


def reference(embeddings, coarse_ids, fine_ids, coarse_old, fine_old):
    values = embeddings.astype(jnp.float32)
    ones_rows = jnp.ones((embeddings.shape[0],), jnp.float32)
    fine_index = coarse_ids * F + fine_ids
    fine_sums = jax.ops.segment_sum(values, fine_index, num_segments=K * F)
    fine_counts = jax.ops.segment_sum(ones_rows, fine_index, num_segments=K * F)
    fine_flat = (fine_old.reshape(K * F, D) + fine_sums) / (1.0 + fine_counts)[:, None]
    coarse_sums = jax.ops.segment_sum(values, coarse_ids, num_segments=K)
    coarse_counts = jax.ops.segment_sum(ones_rows, coarse_ids, num_segments=K)
    coarse_new = (coarse_old + coarse_sums) / (1.0 + coarse_counts)[:, None]
    picked = fine_flat[fine_index]
    diff = values - picked
    distances = jnp.mean(diff * diff, axis=1)
    return coarse_new, fine_flat.reshape(K, F, D), distances
```

```python
import functools

import jax
import jax.numpy as jnp
from jax import lax
from jax.experimental import pallas as pl
from jax.experimental.pallas import tpu as pltpu
from jax.sharding import PartitionSpec as P


AXES = ("rows", "grp")
SLOTS = 4
LANES = 128


def log2(n):
    assert n & (n - 1) == 0
    return n.bit_length() - 1


def iota(shape, dim):
    return lax.broadcasted_iota(jnp.int32, shape, dim)


def pack_kernel(coarse_ref, fine_ref, emb_ref, msg_ref, pos_ref, hot_ref, wide_ref, *, dests, groups, kc, fg):
    rows, width = emb_ref.shape
    lane_groups = width // LANES
    per_msg = SLOTS * lane_groups + 2
    coarse, fine = coarse_ref[...], fine_ref[...]
    dest = (coarse >> log2(kc)) * groups + (fine >> log2(fg))
    local = ((coarse & (kc - 1)) << log2(fg)) + (fine & (fg - 1))
    down = jnp.transpose(jnp.broadcast_to(dest, (LANES, rows)))
    ranks = []
    for j in range(0, rows, LANES):
        before = iota((rows, LANES), 0) < iota((rows, LANES), 1) + j
        same = (down == dest[:, j : j + LANES]) & before
        ranks.append(jnp.sum(jnp.where(same, 1.0, 0.0), axis=0, keepdims=True))
    rank = jnp.concatenate(ranks, axis=1).astype(jnp.int32)
    pos = rank * dests + dest
    pos_ref[...] = pos
    lane = iota((dests, LANES), 1)
    named = jnp.zeros((dests, LANES), jnp.int32)
    mark = (local + 1).astype(jnp.float32)
    for s in range(SLOTS):
        hit = iota((dests, rows), 0) + s * dests == pos
        hot_ref[s * dests : (s + 1) * dests, :] = jnp.where(hit, 1.0, 0.0).astype(jnp.bfloat16)
        found = jnp.sum(jnp.where(hit, mark, 0.0), axis=1, keepdims=True).astype(jnp.int32)
        named = jnp.where(lane == s, found, named)
    named = named - 1
    wide_ref[pl.ds(SLOTS * lane_groups, dests, stride=per_msg), :] = (named >> log2(fg)).astype(jnp.float32)
    wide_ref[pl.ds(SLOTS * lane_groups + 1, dests, stride=per_msg), :] = (named & (fg - 1)).astype(jnp.float32)
    step = 2 * LANES
    for n in range(width // step):
        got = jnp.dot(hot_ref[...], emb_ref[:, n * step : (n + 1) * step], preferred_element_type=jnp.float32)
        for h in range(2):
            for s in range(SLOTS):
                wide_ref[pl.ds(s * lane_groups + 2 * n + h, dests, stride=per_msg), :] = got[
                    s * dests : (s + 1) * dests, h * LANES : (h + 1) * LANES
                ]
    msg_ref[...] = wide_ref[...].astype(jnp.bfloat16)


def update_kernel(msg_ref, old_ref, new_ref, coarse_ref, x_ref, key_ref, wide_ref, mem_ref, *, dests, kc, fg):
    cells, width = old_ref.shape
    lane_groups = width // LANES
    per_msg = SLOTS * lane_groups + 2
    slots = SLOTS * dests
    wide_ref[...] = msg_ref[...].astype(jnp.float32)
    high = wide_ref[pl.ds(SLOTS * lane_groups, dests, stride=per_msg), :]
    low = wide_ref[pl.ds(SLOTS * lane_groups + 1, dests, stride=per_msg), :]
    key = high * fg + low
    key_ref[...] = key
    across = jnp.transpose(key)
    keys = jnp.concatenate([across[s : s + 1, :] for s in range(SLOTS)], axis=1).astype(jnp.int32)
    for s in range(SLOTS):
        for g in range(lane_groups):
            part = wide_ref[pl.ds(s * lane_groups + g, dests, stride=per_msg), :]
            x_ref[s * dests : (s + 1) * dests, g * LANES : (g + 1) * LANES] = part.astype(jnp.bfloat16)
    member = jnp.where(iota((cells, slots), 0) == keys, 1.0, 0.0)
    mem_ref[:cells, :] = member.astype(jnp.bfloat16)
    counts = jnp.sum(member, axis=1, keepdims=True)
    member = jnp.where(iota((kc, slots), 0) == (keys >> log2(fg)), 1.0, 0.0)
    mem_ref[cells:, :] = member.astype(jnp.bfloat16)
    coarse_counts = jnp.sum(member, axis=1, keepdims=True)
    coarse_ref[:, width:] = jnp.broadcast_to(coarse_counts, (kc, LANES))
    step = 2 * LANES
    for n in range(width // step):
        at = slice(n * step, (n + 1) * step)
        sums = jnp.dot(mem_ref[...], x_ref[:, at], preferred_element_type=jnp.float32)
        new_ref[:, at] = (old_ref[:, at] + sums[:cells]) / (1.0 + counts)
        coarse_ref[:, at] = sums[cells:]


def distance_kernel(x_ref, new_ref, key_ref, dist_ref, hot_ref, acc_ref, *, dests):
    cells, width = new_ref.shape
    key = key_ref[...].astype(jnp.int32)
    for s in range(SLOTS):
        hit = iota((dests, cells), 1) == key[:, s : s + 1]
        hot_ref[s * dests : (s + 1) * dests, :] = jnp.where(hit, 1.0, 0.0).astype(jnp.bfloat16)
    step = 2 * LANES
    for n in range(width // step):
        at = slice(n * step, (n + 1) * step)
        new = new_ref[:, at]
        top = new.astype(jnp.bfloat16)
        rest = new - top.astype(jnp.float32)
        mid = rest.astype(jnp.bfloat16)
        end = (rest - mid.astype(jnp.float32)).astype(jnp.bfloat16)
        hot = hot_ref[...]
        picked = jnp.dot(hot, top, preferred_element_type=jnp.float32)
        picked += jnp.dot(hot, mid, preferred_element_type=jnp.float32)
        picked += jnp.dot(hot, end, preferred_element_type=jnp.float32)
        diff = x_ref[:, at].astype(jnp.float32) - picked
        diff = diff * diff
        both = diff[:, :LANES] + diff[:, LANES:]
        if n == 0:
            acc_ref[...] = both
        else:
            acc_ref[...] += both
    for s in range(SLOTS):
        total = jnp.sum(acc_ref[s * dests : (s + 1) * dests, :], axis=1, keepdims=True)
        dist_ref[:, s : s + 1] = total * (1.0 / width)


def finish_kernel(back_ref, pos_ref, out_ref, *, dests):
    pos = pos_ref[...]
    total = jnp.zeros(pos.shape, jnp.float32)
    for s in range(SLOTS):
        hit = iota((dests, pos.shape[1]), 0) + s * dests == pos
        total += jnp.sum(jnp.where(hit, back_ref[:, s : s + 1], 0.0), axis=0, keepdims=True)
    out_ref[...] = total


def call(kernel, outs, scratch=(), limit=24 << 20):
    return pl.pallas_call(
        kernel,
        out_shape=outs,
        scratch_shapes=list(scratch),
        compiler_params=pltpu.CompilerParams(vmem_limit_bytes=limit),
    )


def on_device(embeddings, coarse_ids, fine_ids, coarse_old, fine_old):
    groups = lax.axis_size("grp")
    dests = lax.axis_size("rows") * groups
    rows, width = embeddings.shape
    kc, fg = fine_old.shape[:2]
    cells, slots = kc * fg, SLOTS * dests
    per_msg = SLOTS * (width // LANES) + 2
    f32, bf16 = jnp.float32, jnp.bfloat16
    shape = jax.ShapeDtypeStruct
    msg, pos = call(
        functools.partial(pack_kernel, dests=dests, groups=groups, kc=kc, fg=fg),
        (shape((dests * per_msg, LANES), bf16), shape((1, rows), jnp.int32)),
        (pltpu.VMEM((slots, rows), bf16), pltpu.VMEM((dests * per_msg, LANES), f32)),
    )(coarse_ids.reshape(1, rows), fine_ids.reshape(1, rows), embeddings)
    msg = lax.all_to_all(msg.reshape(dests, per_msg // 2, 2, LANES), AXES, 0, 0, tiled=True)
    new, coarse, x, key = call(
        functools.partial(update_kernel, dests=dests, kc=kc, fg=fg),
        (
            shape((cells, width), f32),
            shape((kc, width + LANES), f32),
            shape((slots, width), bf16),
            shape((dests, LANES), f32),
        ),
        (pltpu.VMEM((dests * per_msg, LANES), f32), pltpu.VMEM((cells + kc, slots), bf16)),
    )(msg.reshape(dests * per_msg, LANES), fine_old.reshape(cells, width))
    coarse = lax.all_to_all(coarse.reshape(groups, kc // groups, width + LANES), "grp", 0, 0, tiled=True)
    dist = call(
        functools.partial(distance_kernel, dests=dests),
        shape((dests, SLOTS), f32),
        (pltpu.VMEM((slots, cells), bf16), pltpu.VMEM((slots, LANES), f32)),
    )(x, new, key)
    back = lax.all_to_all(dist, AXES, 0, 0, tiled=True)
    coarse = jnp.sum(coarse, axis=0)
    coarse_new = (coarse_old + coarse[:, :width]) / (1.0 + coarse[:, width : width + 1])
    distances = call(
        functools.partial(finish_kernel, dests=dests),
        shape((1, rows), f32),
    )(back, pos)
    return (coarse_new, new.reshape(fine_old.shape), distances.reshape(rows))


def solution(mesh):
    return jax.shard_map(
        on_device,
        mesh=mesh,
        in_specs=(
            P(AXES, None),
            P(AXES),
            P(AXES),
            P(AXES, None),
            P("rows", "grp", None),
        ),
        out_specs=(P(AXES, None), P("rows", "grp", None), P(AXES)),
        check_vma=False,
    )
```

```python
import functools

import jax
import jax.numpy as jnp
from jax import lax
from jax.experimental import pallas as pl
from jax.experimental.pallas import tpu as pltpu
from jax.sharding import PartitionSpec as P


AXES = ("rows", "grp")
SLOTS = 4
LANES = 128


def log2(n):
    assert n & (n - 1) == 0
    return n.bit_length() - 1


def iota(shape, dim):
    return lax.broadcasted_iota(jnp.int32, shape, dim)


def pack_kernel(
    coarse_hbm,
    fine_hbm,
    emb_hbm,
    msg_ref,
    pos_ref,
    coarse_ref,
    fine_ref,
    emb_ref,
    sems,
    hot_ref,
    wide_ref,
    *,
    dests,
    groups,
    kc,
    fg,
):
    coarse_copy = pltpu.make_async_copy(coarse_hbm, coarse_ref, sems.at[0])
    fine_copy = pltpu.make_async_copy(fine_hbm, fine_ref, sems.at[1])
    emb_copy = pltpu.make_async_copy(emb_hbm, emb_ref, sems.at[2])
    coarse_copy.start()
    fine_copy.start()
    emb_copy.start()
    rows, width = emb_ref.shape
    lane_groups = width // LANES
    per_msg = SLOTS * lane_groups + 2
    coarse_copy.wait()
    fine_copy.wait()
    coarse, fine = coarse_ref[...], fine_ref[...]
    dest = (coarse >> log2(kc)) * groups + (fine >> log2(fg))
    local = ((coarse & (kc - 1)) << log2(fg)) + (fine & (fg - 1))
    down = jnp.transpose(jnp.broadcast_to(dest, (LANES, rows)))
    ranks = []
    for j in range(0, rows, LANES):
        before = iota((rows, LANES), 0) < iota((rows, LANES), 1) + j
        same = (down == dest[:, j : j + LANES]) & before
        ranks.append(jnp.sum(jnp.where(same, 1.0, 0.0), axis=0, keepdims=True))
    rank = jnp.concatenate(ranks, axis=1).astype(jnp.int32)
    pos = rank * dests + dest
    pos_ref[...] = pos
    lane = iota((dests, LANES), 1)
    named = jnp.zeros((dests, LANES), jnp.int32)
    mark = (local + 1).astype(jnp.float32)
    for s in range(SLOTS):
        hit = iota((dests, rows), 0) + s * dests == pos
        hot_ref[s * dests : (s + 1) * dests, :] = jnp.where(hit, 1.0, 0.0).astype(jnp.bfloat16)
        found = jnp.sum(jnp.where(hit, mark, 0.0), axis=1, keepdims=True).astype(jnp.int32)
        named = jnp.where(lane == s, found, named)
    named = named - 1
    wide_ref[pl.ds(SLOTS * lane_groups, dests, stride=per_msg), :] = (named >> log2(fg)).astype(jnp.float32)
    wide_ref[pl.ds(SLOTS * lane_groups + 1, dests, stride=per_msg), :] = (named & (fg - 1)).astype(jnp.float32)
    emb_copy.wait()
    step = 2 * LANES
    for n in range(width // step):
        got = jnp.dot(hot_ref[...], emb_ref[:, n * step : (n + 1) * step], preferred_element_type=jnp.float32)
        for h in range(2):
            for s in range(SLOTS):
                wide_ref[pl.ds(s * lane_groups + 2 * n + h, dests, stride=per_msg), :] = got[
                    s * dests : (s + 1) * dests, h * LANES : (h + 1) * LANES
                ]
    msg_ref[...] = wide_ref[...].astype(jnp.bfloat16)


def update_kernel(msg_ref, old_ref, new_ref, keep_ref, send_ref, x_ref, key_ref, wide_ref, mem_ref, *, dests, groups, kc, fg):
    cells, width = old_ref.shape
    lane_groups = width // LANES
    per_msg = SLOTS * lane_groups + 2
    slots = SLOTS * dests
    wide_ref[...] = msg_ref[...].astype(jnp.float32)
    high = wide_ref[pl.ds(SLOTS * lane_groups, dests, stride=per_msg), :]
    low = wide_ref[pl.ds(SLOTS * lane_groups + 1, dests, stride=per_msg), :]
    key = high * fg + low
    key_ref[...] = key
    across = jnp.transpose(key)
    keys = jnp.concatenate([across[s : s + 1, :] for s in range(SLOTS)], axis=1).astype(jnp.int32)
    for s in range(SLOTS):
        for g in range(lane_groups):
            part = wide_ref[pl.ds(s * lane_groups + g, dests, stride=per_msg), :]
            x_ref[s * dests : (s + 1) * dests, g * LANES : (g + 1) * LANES] = part.astype(jnp.bfloat16)
    member = jnp.where(iota((cells, slots), 0) == keys, 1.0, 0.0)
    mem_ref[:cells, :] = member.astype(jnp.bfloat16)
    counts = jnp.sum(member, axis=1, keepdims=True)
    block = iota((kc, slots), 0) >> log2(kc // groups)
    block = sum(((block >> b) & 1) << (log2(groups) - 1 - b) for b in range(log2(groups)))
    owned = ((block ^ lax.axis_index("grp")) << log2(kc // groups)) + (iota((kc, slots), 0) & (kc // groups - 1))
    member = jnp.where(owned == (keys >> log2(fg)), 1.0, 0.0)
    mem_ref[cells:, :] = member.astype(jnp.bfloat16)
    coarse_counts = jnp.sum(member, axis=1, keepdims=True)
    coarse_counts = jnp.broadcast_to(coarse_counts, (kc, LANES))
    keep_ref[:, width:] = coarse_counts[: kc // 2]
    send_ref[:, width:] = coarse_counts[kc // 2 :]
    step = 2 * LANES
    for n in range(width // step):
        at = slice(n * step, (n + 1) * step)
        sums = jnp.dot(mem_ref[...], x_ref[:, at], preferred_element_type=jnp.float32)
        new_ref[:, at] = (old_ref[:, at] + sums[:cells]) / (1.0 + counts)
        keep_ref[:, at] = sums[cells : cells + kc // 2]
        send_ref[:, at] = sums[cells + kc // 2 :]


def distance_kernel(x_ref, new_ref, key_ref, dist_ref, out_hbm, hot_ref, acc_ref, sem, *, dests):
    out_copy = pltpu.make_async_copy(new_ref, out_hbm, sem)
    out_copy.start()
    cells, width = new_ref.shape
    key = key_ref[...].astype(jnp.int32)
    for s in range(SLOTS):
        hit = iota((dests, cells), 1) == key[:, s : s + 1]
        hot_ref[s * dests : (s + 1) * dests, :] = jnp.where(hit, 1.0, 0.0).astype(jnp.bfloat16)
    step = 2 * LANES
    for n in range(width // step):
        at = slice(n * step, (n + 1) * step)
        new = new_ref[:, at]
        top = new.astype(jnp.bfloat16)
        rest = new - top.astype(jnp.float32)
        mid = rest.astype(jnp.bfloat16)
        end = (rest - mid.astype(jnp.float32)).astype(jnp.bfloat16)
        hot = hot_ref[...]
        picked = jnp.dot(hot, top, preferred_element_type=jnp.float32)
        picked += jnp.dot(hot, mid, preferred_element_type=jnp.float32)
        picked += jnp.dot(hot, end, preferred_element_type=jnp.float32)
        diff = x_ref[:, at].astype(jnp.float32) - picked
        diff = diff * diff
        both = diff[:, :LANES] + diff[:, LANES:]
        if n == 0:
            acc_ref[...] = both
        else:
            acc_ref[...] += both
    for s in range(SLOTS):
        total = jnp.sum(acc_ref[s * dests : (s + 1) * dests, :], axis=1, keepdims=True)
        dist_ref[:, s : s + 1] = total * (1.0 / width)
    out_copy.wait()


def finish_kernel(back_ref, pos_ref, out_ref, *, dests):
    pos = pos_ref[...]
    total = jnp.zeros(pos.shape, jnp.float32)
    for s in range(SLOTS):
        hit = iota((dests, pos.shape[1]), 0) + s * dests == pos
        total += jnp.sum(jnp.where(hit, back_ref[:, s : s + 1], 0.0), axis=0, keepdims=True)
    out_ref[...] = total


def call(kernel, outs, scratch=(), limit=24 << 20, **specs):
    return pl.pallas_call(
        kernel,
        out_shape=outs,
        **specs,
        scratch_shapes=list(scratch),
        compiler_params=pltpu.CompilerParams(vmem_limit_bytes=limit),
    )


def on_device(embeddings, coarse_ids, fine_ids, coarse_old, fine_old):
    groups = lax.axis_size("grp")
    dests = lax.axis_size("rows") * groups
    rows, width = embeddings.shape
    kc, fg = fine_old.shape[:2]
    cells, slots = kc * fg, SLOTS * dests
    per_msg = SLOTS * (width // LANES) + 2
    f32, bf16 = jnp.float32, jnp.bfloat16
    shape = jax.ShapeDtypeStruct
    ids = coarse_ids.reshape(1, rows), fine_ids.reshape(1, rows)
    msg, pos = call(
        functools.partial(pack_kernel, dests=dests, groups=groups, kc=kc, fg=fg),
        (shape((dests * per_msg, LANES), bf16), shape((1, rows), jnp.int32)),
        (
            pltpu.VMEM((1, rows), jnp.int32),
            pltpu.VMEM((1, rows), jnp.int32),
            pltpu.VMEM((rows, width), bf16),
            pltpu.SemaphoreType.DMA((3,)),
            pltpu.VMEM((slots, rows), bf16),
            pltpu.VMEM((dests * per_msg, LANES), f32),
        ),
        in_specs=[pl.BlockSpec(memory_space=pltpu.HBM)] * 3,
    )(*(pltpu.with_memory_space_constraint(a, pltpu.HBM) for a in (ids[0], ids[1], embeddings)))
    msg = lax.all_to_all(msg.reshape(dests, per_msg // 2, 2, LANES), AXES, 0, 0, tiled=True)
    new, coarse, away, x, key = call(
        functools.partial(update_kernel, dests=dests, groups=groups, kc=kc, fg=fg),
        (
            shape((cells, width), f32),
            shape((kc // 2, width + LANES), f32),
            shape((kc // 2, width + LANES), f32),
            shape((slots, width), bf16),
            shape((dests, LANES), f32),
        ),
        (pltpu.VMEM((dests * per_msg, LANES), f32), pltpu.VMEM((cells + kc, slots), bf16)),
    )(msg.reshape(dests * per_msg, LANES), fine_old.reshape(cells, width))
    dist, new = call(
        functools.partial(distance_kernel, dests=dests),
        (shape((dests, SLOTS), f32), shape((cells, width), f32)),
        (pltpu.VMEM((slots, cells), bf16), pltpu.VMEM((slots, LANES), f32), pltpu.SemaphoreType.DMA(())),
        out_specs=(pl.BlockSpec(memory_space=pltpu.VMEM), pl.BlockSpec(memory_space=pltpu.HBM)),
    )(x, new, key)
    back = lax.all_to_all(dist, AXES, 0, 0, tiled=True)
    for bit in range(log2(groups)):
        pairs = [(g, g ^ (1 << bit)) for g in range(groups)]
        coarse = coarse + lax.ppermute(away, "grp", pairs)
        if bit < log2(groups) - 1:
            half = coarse.shape[0] // 2
            coarse, away = coarse[:half], coarse[half:]
    coarse_new = (coarse_old + coarse[:, :width]) / (1.0 + coarse[:, width : width + 1])
    distances = call(
        functools.partial(finish_kernel, dests=dests),
        shape((1, rows), f32),
    )(back, pos)
    return (coarse_new, new.reshape(fine_old.shape), distances.reshape(rows))


def solution(mesh):
    return jax.shard_map(
        on_device,
        mesh=mesh,
        in_specs=(
            P(AXES, None),
            P(AXES),
            P(AXES),
            P(AXES, None),
            P("rows", "grp", None),
        ),
        out_specs=(P(AXES, None), P("rows", "grp", None), P(AXES)),
        check_vma=False,
    )
```

```python
import functools

import jax
import jax.numpy as jnp
from jax import lax
from jax.experimental import pallas as pl
from jax.experimental.pallas import tpu as pltpu
from jax.sharding import PartitionSpec as P


AXES = ("rows", "grp")
SLOTS = 4
LANES = 128


def log2(n):
    assert n & (n - 1) == 0
    return n.bit_length() - 1


def iota(shape, dim):
    return lax.broadcasted_iota(jnp.int32, shape, dim)


def pack_kernel(
    coarse_hbm,
    fine_hbm,
    emb_hbm,
    msg_ref,
    pos_ref,
    coarse_ref,
    fine_ref,
    emb_ref,
    sems,
    hot_ref,
    wide_ref,
    *,
    dests,
    groups,
    kc,
    fg,
):
    coarse_copy = pltpu.make_async_copy(coarse_hbm, coarse_ref, sems.at[0])
    fine_copy = pltpu.make_async_copy(fine_hbm, fine_ref, sems.at[1])
    emb_copy = pltpu.make_async_copy(emb_hbm, emb_ref, sems.at[2])
    coarse_copy.start()
    fine_copy.start()
    emb_copy.start()
    rows, width = emb_ref.shape
    lane_groups = width // LANES
    per_msg = SLOTS * lane_groups + 2
    coarse_copy.wait()
    fine_copy.wait()
    coarse, fine = coarse_ref[...], fine_ref[...]
    dest = (coarse >> log2(kc)) * groups + (fine >> log2(fg))
    local = ((coarse & (kc - 1)) << log2(fg)) + (fine & (fg - 1))
    down = jnp.transpose(jnp.broadcast_to(dest, (LANES, rows)))
    ranks = []
    for j in range(0, rows, LANES):
        before = iota((rows, LANES), 0) < iota((rows, LANES), 1) + j
        same = (down == dest[:, j : j + LANES]) & before
        ranks.append(jnp.sum(jnp.where(same, 1.0, 0.0), axis=0, keepdims=True))
    rank = jnp.concatenate(ranks, axis=1).astype(jnp.int32)
    pos = rank * dests + dest
    pos_ref[...] = pos
    lane = iota((dests, LANES), 1)
    named = jnp.zeros((dests, LANES), jnp.int32)
    mark = (local + 1).astype(jnp.float32)
    for s in range(SLOTS):
        hit = iota((dests, rows), 0) + s * dests == pos
        hot_ref[s * dests : (s + 1) * dests, :] = jnp.where(hit, 1.0, 0.0).astype(jnp.bfloat16)
        found = jnp.sum(jnp.where(hit, mark, 0.0), axis=1, keepdims=True).astype(jnp.int32)
        named = jnp.where(lane == s, found, named)
    named = named - 1
    wide_ref[pl.ds(SLOTS * lane_groups, dests, stride=per_msg), :] = (named >> log2(fg)).astype(jnp.float32)
    wide_ref[pl.ds(SLOTS * lane_groups + 1, dests, stride=per_msg), :] = (named & (fg - 1)).astype(jnp.float32)
    emb_copy.wait()
    step = 2 * LANES
    for n in range(width // step):
        got = jnp.dot(hot_ref[...], emb_ref[:, n * step : (n + 1) * step], preferred_element_type=jnp.float32)
        for h in range(2):
            for s in range(SLOTS):
                wide_ref[pl.ds(s * lane_groups + 2 * n + h, dests, stride=per_msg), :] = got[
                    s * dests : (s + 1) * dests, h * LANES : (h + 1) * LANES
                ]
    msg_ref[...] = wide_ref[...].astype(jnp.bfloat16)


def update_kernel(
    msg_ref,
    old_ref,
    keep_ref,
    send_ref,
    dist_ref,
    out_hbm,
    wide_ref,
    x_ref,
    mem_ref,
    new_ref,
    tall_ref,
    key_ref,
    key_smem,
    gap_ref,
    sems,
    *,
    dests,
    groups,
    kc,
    fg,
):
    cells, width = old_ref.shape
    lane_groups = width // LANES
    per_msg = SLOTS * lane_groups + 2
    slots = SLOTS * dests
    wide_ref[...] = msg_ref[...].astype(jnp.float32)
    high = wide_ref[pl.ds(SLOTS * lane_groups, dests, stride=per_msg), :]
    low = wide_ref[pl.ds(SLOTS * lane_groups + 1, dests, stride=per_msg), :]
    across = jnp.transpose(high * fg + low)[:8].astype(jnp.int32)
    key_ref[...] = jnp.minimum(jnp.maximum(across, 0), cells - 1)
    key_copy = pltpu.make_async_copy(key_ref, key_smem, sems.at[0])
    key_copy.start()
    keys = jnp.concatenate([across[s : s + 1, :] for s in range(SLOTS)], axis=1)
    for s in range(SLOTS):
        for g in range(lane_groups):
            part = wide_ref[pl.ds(s * lane_groups + g, dests, stride=per_msg), :]
            x_ref[s * dests : (s + 1) * dests, g * LANES : (g + 1) * LANES] = part.astype(jnp.bfloat16)
    member = jnp.where(iota((cells, slots), 0) == keys, 1.0, 0.0)
    mem_ref[:cells, :] = member.astype(jnp.bfloat16)
    counts = jnp.sum(member, axis=1, keepdims=True)
    block = iota((kc, slots), 0) >> log2(kc // groups)
    block = sum(((block >> b) & 1) << (log2(groups) - 1 - b) for b in range(log2(groups)))
    owned = ((block ^ lax.axis_index("grp")) << log2(kc // groups)) + (iota((kc, slots), 0) & (kc // groups - 1))
    member = jnp.where(owned == (keys >> log2(fg)), 1.0, 0.0)
    mem_ref[cells:, :] = member.astype(jnp.bfloat16)
    coarse_counts = jnp.sum(member, axis=1, keepdims=True)
    coarse_counts = jnp.broadcast_to(coarse_counts, (kc, LANES))
    keep_ref[:, width:] = coarse_counts[: kc // 2]
    send_ref[:, width:] = coarse_counts[kc // 2 :]
    step = 2 * LANES
    for n in range(width // step):
        at = slice(n * step, (n + 1) * step)
        sums = jnp.dot(mem_ref[...], x_ref[:, at], preferred_element_type=jnp.float32)
        new = (old_ref[:, at] + sums[:cells]) / (1.0 + counts)
        new_ref[:, at] = new
        for h in range(2):
            tall_ref[pl.ds(2 * n + h, cells, stride=lane_groups), :] = new[:, h * LANES : (h + 1) * LANES]
        keep_ref[:, at] = sums[cells : cells + kc // 2]
        send_ref[:, at] = sums[cells + kc // 2 :]
    out_copy = pltpu.make_async_copy(new_ref, out_hbm, sems.at[1])
    out_copy.start()
    key_copy.wait()
    unroll = 8

    @pl.loop(0, dests // unroll)
    def _(i):
        base = pl.multiple_of(i * (unroll * per_msg), 8)
        for u in range(unroll):
            for s in range(SLOTS):
                key = key_smem[s, i * unroll + u]
                near = tall_ref[pl.ds(pl.multiple_of(key * lane_groups, 8), lane_groups), :]
                row = wide_ref[pl.ds(base + u * per_msg + s * lane_groups, lane_groups), :]
                gap = row - near
                at = (s * dests + u) * lane_groups + i * (unroll * lane_groups)
                gap_ref[pl.ds(pl.multiple_of(at, 8), lane_groups), :] = gap * gap

    for s in range(SLOTS):
        total = gap_ref[pl.ds(s * dests * lane_groups, dests, stride=lane_groups), :]
        for j in range(1, lane_groups):
            total += gap_ref[pl.ds(s * dests * lane_groups + j, dests, stride=lane_groups), :]
        dist_ref[:, s : s + 1] = jnp.sum(total, axis=1, keepdims=True) * (1.0 / width)
    out_copy.wait()


def finish_kernel(back_ref, pos_ref, out_ref, *, dests):
    pos = pos_ref[...]
    total = jnp.zeros(pos.shape, jnp.float32)
    for s in range(SLOTS):
        hit = iota((dests, pos.shape[1]), 0) + s * dests == pos
        total += jnp.sum(jnp.where(hit, back_ref[:, s : s + 1], 0.0), axis=0, keepdims=True)
    out_ref[...] = total


def call(kernel, outs, scratch=(), limit=24 << 20, **specs):
    return pl.pallas_call(
        kernel,
        out_shape=outs,
        **specs,
        scratch_shapes=list(scratch),
        compiler_params=pltpu.CompilerParams(vmem_limit_bytes=limit),
    )


def on_device(embeddings, coarse_ids, fine_ids, coarse_old, fine_old):
    groups = lax.axis_size("grp")
    dests = lax.axis_size("rows") * groups
    rows, width = embeddings.shape
    kc, fg = fine_old.shape[:2]
    cells, slots = kc * fg, SLOTS * dests
    per_msg = SLOTS * (width // LANES) + 2
    f32, bf16 = jnp.float32, jnp.bfloat16
    shape = jax.ShapeDtypeStruct
    ids = coarse_ids.reshape(1, rows), fine_ids.reshape(1, rows)
    msg, pos = call(
        functools.partial(pack_kernel, dests=dests, groups=groups, kc=kc, fg=fg),
        (shape((dests * per_msg, LANES), bf16), shape((1, rows), jnp.int32)),
        (
            pltpu.VMEM((1, rows), jnp.int32),
            pltpu.VMEM((1, rows), jnp.int32),
            pltpu.VMEM((rows, width), bf16),
            pltpu.SemaphoreType.DMA((3,)),
            pltpu.VMEM((slots, rows), bf16),
            pltpu.VMEM((dests * per_msg, LANES), f32),
        ),
        in_specs=[pl.BlockSpec(memory_space=pltpu.HBM)] * 3,
    )(*(pltpu.with_memory_space_constraint(a, pltpu.HBM) for a in (ids[0], ids[1], embeddings)))
    msg = lax.all_to_all(msg.reshape(dests, per_msg // 2, 2, LANES), AXES, 0, 0, tiled=True)
    coarse, away, dist, new = call(
        functools.partial(update_kernel, dests=dests, groups=groups, kc=kc, fg=fg),
        (
            shape((kc // 2, width + LANES), f32),
            shape((kc // 2, width + LANES), f32),
            shape((dests, SLOTS), f32),
            shape((cells, width), f32),
        ),
        (
            pltpu.VMEM((dests * per_msg, LANES), f32),
            pltpu.VMEM((slots, width), bf16),
            pltpu.VMEM((cells + kc, slots), bf16),
            pltpu.VMEM((cells, width), f32),
            pltpu.VMEM((cells * width // LANES, LANES), f32),
            pltpu.VMEM((8, dests), jnp.int32),
            pltpu.SMEM((8, dests), jnp.int32),
            pltpu.VMEM((slots * width // LANES, LANES), f32),
            pltpu.SemaphoreType.DMA((2,)),
        ),
        32 << 20,
        out_specs=(pl.BlockSpec(memory_space=pltpu.VMEM),) * 3 + (pl.BlockSpec(memory_space=pltpu.HBM),),
    )(msg.reshape(dests * per_msg, LANES), fine_old.reshape(cells, width))
    back = lax.all_to_all(dist, AXES, 0, 0, tiled=True)
    rounds = log2(groups)
    coarse = coarse + lax.ppermute(away, "grp", [(g, g ^ 1) for g in range(groups)])
    owned = kc // groups
    parts = [coarse[:owned]]
    for p in range(1, groups // 2):
        partner = sum(((p >> b) & 1) << (rounds - 1 - b) for b in range(rounds))
        parts.append(lax.ppermute(coarse[p * owned : (p + 1) * owned], "grp", [(g, g ^ partner) for g in range(groups)]))
    coarse = functools.reduce(jnp.add, parts)
    coarse_new = (coarse_old + coarse[:, :width]) / (1.0 + coarse[:, width : width + 1])
    distances = call(
        functools.partial(finish_kernel, dests=dests),
        shape((1, rows), f32),
    )(back, pos)
    return (coarse_new, new.reshape(fine_old.shape), distances.reshape(rows))


def solution(mesh):
    return jax.shard_map(
        on_device,
        mesh=mesh,
        in_specs=(
            P(AXES, None),
            P(AXES),
            P(AXES),
            P(AXES, None),
            P("rows", "grp", None),
        ),
        out_specs=(P(AXES, None), P("rows", "grp", None), P(AXES)),
        check_vma=False,
    )
```

```python
import functools

import jax
import jax.numpy as jnp
from jax import lax
from jax.experimental import pallas as pl
from jax.experimental.pallas import tpu as pltpu
from jax.sharding import PartitionSpec as P


AXES = ("rows", "grp")
SLOTS = 4
LANES = 128


def log2(n):
    assert n & (n - 1) == 0
    return n.bit_length() - 1


def iota(shape, dim):
    return lax.broadcasted_iota(jnp.int32, shape, dim)


def pack_kernel(
    coarse_hbm,
    fine_hbm,
    emb_hbm,
    msg_ref,
    pos_ref,
    coarse_ref,
    fine_ref,
    emb_ref,
    sems,
    hot_ref,
    wide_ref,
    *,
    dests,
    groups,
    kc,
    fg,
):
    coarse_copy = pltpu.make_async_copy(coarse_hbm, coarse_ref, sems.at[0])
    fine_copy = pltpu.make_async_copy(fine_hbm, fine_ref, sems.at[1])
    emb_copy = pltpu.make_async_copy(emb_hbm, emb_ref, sems.at[2])
    coarse_copy.start()
    fine_copy.start()
    emb_copy.start()
    rows, width = emb_ref.shape
    lane_groups = width // LANES
    per_msg = SLOTS * lane_groups + 2
    coarse_copy.wait()
    fine_copy.wait()
    coarse, fine = coarse_ref[...], fine_ref[...]
    dest = (coarse >> log2(kc)) * groups + (fine >> log2(fg))
    local = ((coarse & (kc - 1)) << log2(fg)) + (fine & (fg - 1))
    down = jnp.transpose(jnp.broadcast_to(dest, (LANES, rows)))
    ranks = []
    for j in range(0, rows, LANES):
        before = iota((rows, LANES), 0) < iota((rows, LANES), 1) + j
        same = (down == dest[:, j : j + LANES]) & before
        ranks.append(jnp.sum(jnp.where(same, 1.0, 0.0), axis=0, keepdims=True))
    rank = jnp.concatenate(ranks, axis=1).astype(jnp.int32)
    pos = rank * dests + dest
    pos_ref[...] = pos
    lane = iota((dests, LANES), 1)
    named = jnp.zeros((dests, LANES), jnp.int32)
    mark = (local + 1).astype(jnp.float32)
    for s in range(SLOTS):
        hit = iota((dests, rows), 0) + s * dests == pos
        hot_ref[s * dests : (s + 1) * dests, :] = jnp.where(hit, 1.0, 0.0).astype(jnp.bfloat16)
        found = jnp.sum(jnp.where(hit, mark, 0.0), axis=1, keepdims=True).astype(jnp.int32)
        named = jnp.where(lane == s, found, named)
    named = named - 1
    wide_ref[pl.ds(SLOTS * lane_groups, dests, stride=per_msg), :] = (named >> log2(fg)).astype(jnp.float32)
    wide_ref[pl.ds(SLOTS * lane_groups + 1, dests, stride=per_msg), :] = (named & (fg - 1)).astype(jnp.float32)
    emb_copy.wait()
    step = 2 * LANES
    for n in range(width // step):
        got = jnp.dot(hot_ref[...], emb_ref[:, n * step : (n + 1) * step], preferred_element_type=jnp.float32)
        for h in range(2):
            for s in range(SLOTS):
                wide_ref[pl.ds(s * lane_groups + 2 * n + h, dests, stride=per_msg), :] = got[
                    s * dests : (s + 1) * dests, h * LANES : (h + 1) * LANES
                ]
    msg_ref[...] = wide_ref[...].astype(jnp.bfloat16)


def fold(parts):
    parts = [parts[u ^ 3] for u in range(8)]
    row = iota(parts[0].shape, 0)
    low = row < 4
    parts = [
        jnp.where(low, a, b) + pltpu.roll(jnp.where(low, b, a), 4, 0) for a, b in zip(parts[:4], parts[4:])
    ]
    for k in (2, 1):
        kept = (row & k) != 0
        parts = [
            jnp.where(kept, a, b) + jnp.where(kept, pltpu.roll(a, k, 0), pltpu.roll(b, 8 - k, 0))
            for a, b in zip(parts[:k], parts[k:])
        ]
    return parts[0]


def update_kernel(
    msg_ref,
    old_ref,
    keep_ref,
    send_ref,
    dist_ref,
    out_hbm,
    wide_ref,
    x_ref,
    mem_ref,
    new_ref,
    tall_ref,
    column_ref,
    key_ref,
    key_smem,
    gap_ref,
    sems,
    *,
    dests,
    groups,
    kc,
    fg,
):
    cells, width = old_ref.shape
    lane_groups = width // LANES
    per_msg = SLOTS * lane_groups + 2
    slots = SLOTS * dests
    wide_ref[...] = msg_ref[...].astype(jnp.float32)
    high = wide_ref[pl.ds(SLOTS * lane_groups, dests, stride=per_msg), :]
    low = wide_ref[pl.ds(SLOTS * lane_groups + 1, dests, stride=per_msg), :]
    key = high * fg + low
    column_ref[...] = jnp.minimum(jnp.maximum(key.astype(jnp.int32), 0), cells - 1) * lane_groups
    unroll = 16
    steps = dests // unroll
    near = jnp.zeros((steps, LANES), jnp.int32)
    for u in range(unroll):
        part = column_ref[pl.ds(u, steps, stride=unroll), :]
        if u:
            part = pltpu.roll(part, u * SLOTS, 1)
        near = jnp.where(iota((steps, LANES), 1) >> log2(SLOTS) == u, part, near)
    key_ref[...] = near
    key_copy = pltpu.make_async_copy(key_ref, key_smem, sems.at[0])
    key_copy.start()
    across = jnp.transpose(key)[:8].astype(jnp.int32)
    keys = jnp.concatenate([across[s : s + 1, :] for s in range(SLOTS)], axis=1)
    for s in range(SLOTS):
        for g in range(lane_groups):
            part = wide_ref[pl.ds(s * lane_groups + g, dests, stride=per_msg), :]
            x_ref[s * dests : (s + 1) * dests, g * LANES : (g + 1) * LANES] = part.astype(jnp.bfloat16)
    member = jnp.where(iota((cells, slots), 0) == keys, 1.0, 0.0)
    mem_ref[:cells, :] = member.astype(jnp.bfloat16)
    counts = jnp.sum(member, axis=1, keepdims=True)
    block = iota((kc, slots), 0) >> log2(kc // groups)
    block = sum(((block >> b) & 1) << (log2(groups) - 1 - b) for b in range(log2(groups)))
    owned = ((block ^ lax.axis_index("grp")) << log2(kc // groups)) + (iota((kc, slots), 0) & (kc // groups - 1))
    member = jnp.where(owned == (keys >> log2(fg)), 1.0, 0.0)
    mem_ref[cells:, :] = member.astype(jnp.bfloat16)
    coarse_counts = jnp.sum(member, axis=1, keepdims=True)
    coarse_counts = jnp.broadcast_to(coarse_counts, (kc, LANES))
    keep_ref[:, width:] = coarse_counts[: kc // 2]
    send_ref[:, width:] = coarse_counts[kc // 2 :]
    step = 2 * LANES
    for n in range(width // step):
        at = slice(n * step, (n + 1) * step)
        sums = jnp.dot(mem_ref[...], x_ref[:, at], preferred_element_type=jnp.float32)
        new = (old_ref[:, at] + sums[:cells]) / (1.0 + counts)
        new_ref[:, at] = new
        for h in range(2):
            tall_ref[pl.ds(2 * n + h, cells, stride=lane_groups), :] = new[:, h * LANES : (h + 1) * LANES]
        keep_ref[:, at] = sums[cells : cells + kc // 2]
        send_ref[:, at] = sums[cells + kc // 2 :]
    out_copy = pltpu.make_async_copy(new_ref, out_hbm, sems.at[1])
    out_copy.start()
    key_copy.wait()

    @pl.loop(0, steps)
    def _(i):
        base = pl.multiple_of(i * (unroll * per_msg), 8)
        for s in range(SLOTS):
            for v in range(0, unroll, 8):
                gaps = []
                for u in range(v, v + 8):
                    at = pl.multiple_of(key_smem[i, u * SLOTS + s], 8)
                    row = wide_ref[pl.ds(base + u * per_msg + s * lane_groups, lane_groups), :]
                    gap = row - tall_ref[pl.ds(at, lane_groups), :]
                    gaps.append(gap * gap)
                gap_ref[pl.ds(pl.multiple_of(s * dests + i * unroll + v, 8), 8), :] = fold(gaps)

    for s in range(SLOTS):
        total = jnp.sum(gap_ref[s * dests : (s + 1) * dests, :], axis=1, keepdims=True)
        dist_ref[:, s : s + 1] = total * (1.0 / width)
    out_copy.wait()


def finish_kernel(back_ref, pos_ref, out_ref, *, dests):
    pos = pos_ref[...]
    total = jnp.zeros(pos.shape, jnp.float32)
    for s in range(SLOTS):
        hit = iota((dests, pos.shape[1]), 0) + s * dests == pos
        total += jnp.sum(jnp.where(hit, back_ref[:, s : s + 1], 0.0), axis=0, keepdims=True)
    out_ref[...] = total


def call(kernel, outs, scratch=(), limit=24 << 20, **specs):
    return pl.pallas_call(
        kernel,
        out_shape=outs,
        **specs,
        scratch_shapes=list(scratch),
        compiler_params=pltpu.CompilerParams(vmem_limit_bytes=limit),
    )


def on_device(embeddings, coarse_ids, fine_ids, coarse_old, fine_old):
    groups = lax.axis_size("grp")
    dests = lax.axis_size("rows") * groups
    rows, width = embeddings.shape
    kc, fg = fine_old.shape[:2]
    cells, slots = kc * fg, SLOTS * dests
    per_msg = SLOTS * (width // LANES) + 2
    f32, bf16 = jnp.float32, jnp.bfloat16
    shape = jax.ShapeDtypeStruct
    ids = coarse_ids.reshape(1, rows), fine_ids.reshape(1, rows)
    msg, pos = call(
        functools.partial(pack_kernel, dests=dests, groups=groups, kc=kc, fg=fg),
        (shape((dests * per_msg, LANES), bf16), shape((1, rows), jnp.int32)),
        (
            pltpu.VMEM((1, rows), jnp.int32),
            pltpu.VMEM((1, rows), jnp.int32),
            pltpu.VMEM((rows, width), bf16),
            pltpu.SemaphoreType.DMA((3,)),
            pltpu.VMEM((slots, rows), bf16),
            pltpu.VMEM((dests * per_msg, LANES), f32),
        ),
        in_specs=[pl.BlockSpec(memory_space=pltpu.HBM)] * 3,
    )(*(pltpu.with_memory_space_constraint(a, pltpu.HBM) for a in (ids[0], ids[1], embeddings)))
    msg = lax.all_to_all(msg.reshape(dests, per_msg // 2, 2, LANES), AXES, 0, 0, tiled=True)
    coarse, away, dist, new = call(
        functools.partial(update_kernel, dests=dests, groups=groups, kc=kc, fg=fg),
        (
            shape((kc // 2, width + LANES), f32),
            shape((kc // 2, width + LANES), f32),
            shape((dests, SLOTS), f32),
            shape((cells, width), f32),
        ),
        (
            pltpu.VMEM((dests * per_msg, LANES), f32),
            pltpu.VMEM((slots, width), bf16),
            pltpu.VMEM((cells + kc, slots), bf16),
            pltpu.VMEM((cells, width), f32),
            pltpu.VMEM((cells * width // LANES, LANES), f32),
            pltpu.VMEM((dests, LANES), jnp.int32),
            pltpu.VMEM((dests // 16, LANES), jnp.int32),
            pltpu.SMEM((dests // 16, LANES), jnp.int32),
            pltpu.VMEM((slots, LANES), f32),
            pltpu.SemaphoreType.DMA((2,)),
        ),
        32 << 20,
        out_specs=(pl.BlockSpec(memory_space=pltpu.VMEM),) * 3 + (pl.BlockSpec(memory_space=pltpu.HBM),),
    )(msg.reshape(dests * per_msg, LANES), fine_old.reshape(cells, width))
    back = lax.all_to_all(dist, AXES, 0, 0, tiled=True)
    rounds = log2(groups)
    coarse = coarse + lax.ppermute(away, "grp", [(g, g ^ 1) for g in range(groups)])
    owned = kc // groups
    parts = [coarse[:owned]]
    for p in range(1, groups // 2):
        partner = sum(((p >> b) & 1) << (rounds - 1 - b) for b in range(rounds))
        parts.append(lax.ppermute(coarse[p * owned : (p + 1) * owned], "grp", [(g, g ^ partner) for g in range(groups)]))
    coarse = functools.reduce(jnp.add, parts)
    coarse_new = (coarse_old + coarse[:, :width]) / (1.0 + coarse[:, width : width + 1])
    distances = call(
        functools.partial(finish_kernel, dests=dests),
        shape((1, rows), f32),
    )(back, pos)
    return (coarse_new, new.reshape(fine_old.shape), distances.reshape(rows))


def solution(mesh):
    return jax.shard_map(
        on_device,
        mesh=mesh,
        in_specs=(
            P(AXES, None),
            P(AXES),
            P(AXES),
            P(AXES, None),
            P("rows", "grp", None),
        ),
        out_specs=(P(AXES, None), P("rows", "grp", None), P(AXES)),
        check_vma=False,
    )
```

```python
import functools

import jax
import jax.numpy as jnp
from jax import lax
from jax.experimental import pallas as pl
from jax.experimental.pallas import tpu as pltpu
from jax.sharding import PartitionSpec as P


AXES = ("rows", "grp")
SLOTS = 4
LANES = 128


def log2(n):
    assert n & (n - 1) == 0
    return n.bit_length() - 1


def iota(shape, dim):
    return lax.broadcasted_iota(jnp.int32, shape, dim)


def pack_kernel(
    coarse_hbm,
    fine_hbm,
    emb_hbm,
    msg_ref,
    pos_ref,
    coarse_ref,
    fine_ref,
    emb_ref,
    sems,
    hot_ref,
    wide_ref,
    *,
    dests,
    groups,
    kc,
    fg,
):
    coarse_copy = pltpu.make_async_copy(coarse_hbm, coarse_ref, sems.at[0])
    fine_copy = pltpu.make_async_copy(fine_hbm, fine_ref, sems.at[1])
    emb_copy = pltpu.make_async_copy(emb_hbm, emb_ref, sems.at[2])
    coarse_copy.start()
    fine_copy.start()
    emb_copy.start()
    rows, width = emb_ref.shape
    lane_groups = width // LANES
    per_msg = SLOTS * lane_groups + 2
    part = dests
    coarse_copy.wait()
    fine_copy.wait()
    coarse, fine = coarse_ref[...], fine_ref[...]
    dest = (coarse >> log2(kc)) * groups + (fine >> log2(fg))
    down = jnp.transpose(jnp.broadcast_to(dest, (LANES, rows)))
    ranks = []
    for j in range(0, rows, LANES):
        same = down[: j + LANES] == dest[:, j : j + LANES]
        same = same & (iota((j + LANES, LANES), 0) < iota((j + LANES, LANES), 1) + j)
        ranks.append(jnp.sum(jnp.where(same, 1.0, 0.0), axis=0, keepdims=True))
    rank = jnp.concatenate(ranks, axis=1).astype(jnp.int32)
    pos = rank * dests + dest
    pos_ref[...] = pos
    half = LANES // 2
    names = jnp.where(iota((LANES, rows), 0) < half, (coarse & (kc - 1)) + 1, fine & (fg - 1))
    names = jnp.transpose(names.astype(jnp.float32)).astype(jnp.bfloat16)
    lane = iota((part, LANES), 1)
    step = 2 * LANES
    for p in range(0, dests, part):
        for s in range(SLOTS):
            hit = iota((part, rows), 0) + (s * dests + p) == pos
            hot_ref[p * SLOTS + s * part : p * SLOTS + (s + 1) * part, :] = jnp.where(hit, 1.0, 0.0).astype(jnp.bfloat16)
    for p in range(0, dests, part):
        hot = hot_ref[p * SLOTS : (p + part) * SLOTS, :]
        got = jnp.dot(hot, names, preferred_element_type=jnp.float32)
        named = jnp.zeros((part, LANES), jnp.float32)
        for s in range(SLOTS):
            named = jnp.where(lane & (half - 1) == s, got[s * part : (s + 1) * part], named)
        at = p * per_msg + SLOTS * lane_groups
        wide_ref[pl.ds(at, part, stride=per_msg), :] = named - jnp.where(lane < half, 1.0, 0.0)
        wide_ref[pl.ds(at + 1, part, stride=per_msg), :] = jnp.zeros((part, LANES), jnp.float32)
    emb_copy.wait()
    for p in range(0, dests, part):
        hot = hot_ref[p * SLOTS : (p + part) * SLOTS, :]
        for n in range(width // step):
            got = jnp.dot(hot, emb_ref[:, n * step : (n + 1) * step], preferred_element_type=jnp.float32)
            for h in range(2):
                for s in range(SLOTS):
                    at = p * per_msg + s * lane_groups + 2 * n + h
                    wide_ref[pl.ds(at, part, stride=per_msg), :] = got[s * part : (s + 1) * part, h * LANES : (h + 1) * LANES]
        at = slice(p * per_msg, (p + part) * per_msg)
        msg_ref[at, :] = wide_ref[at, :].astype(jnp.bfloat16)


def fold(parts):
    parts = [parts[u ^ 3] for u in range(8)]
    row = iota(parts[0].shape, 0)
    low = row < 4
    parts = [
        jnp.where(low, a, b) + pltpu.roll(jnp.where(low, b, a), 4, 0) for a, b in zip(parts[:4], parts[4:])
    ]
    for k in (2, 1):
        kept = (row & k) != 0
        parts = [
            jnp.where(kept, a, b) + jnp.where(kept, pltpu.roll(a, k, 0), pltpu.roll(b, 8 - k, 0))
            for a, b in zip(parts[:k], parts[k:])
        ]
    return parts[0]


def update_kernel(
    msg_ref,
    old_ref,
    keep_ref,
    send_ref,
    dist_ref,
    out_hbm,
    wide_ref,
    x_ref,
    mem_ref,
    new_ref,
    tall_ref,
    share_ref,
    column_ref,
    key_ref,
    key_smem,
    gap_ref,
    sems,
    *,
    dests,
    groups,
    kc,
    fg,
):
    cells, width = old_ref.shape
    lane_groups = width // LANES
    per_msg = SLOTS * lane_groups + 2
    slots = SLOTS * dests
    wide_ref[...] = msg_ref[...].astype(jnp.float32)
    names = wide_ref[pl.ds(SLOTS * lane_groups, dests, stride=per_msg), :]
    key = names * fg + pltpu.roll(names, LANES // 2, 1)
    column_ref[...] = jnp.minimum(jnp.maximum(key.astype(jnp.int32), 0), cells - 1) * lane_groups
    unroll = 16
    steps = dests // unroll
    near = jnp.zeros((steps, LANES), jnp.int32)
    for u in range(unroll):
        part = column_ref[pl.ds(u, steps, stride=unroll), :]
        if u:
            part = pltpu.roll(part, u * SLOTS, 1)
        near = jnp.where(iota((steps, LANES), 1) >> log2(SLOTS) == u, part, near)
    key_ref[...] = near
    key_copy = pltpu.make_async_copy(key_ref, key_smem, sems.at[0])
    key_copy.start()
    across = jnp.transpose(key)[:8].astype(jnp.int32)
    keys = jnp.concatenate([across[s : s + 1, :] for s in range(SLOTS)], axis=1)
    for s in range(SLOTS):
        for g in range(lane_groups):
            part = wide_ref[pl.ds(s * lane_groups + g, dests, stride=per_msg), :]
            x_ref[s * dests : (s + 1) * dests, g * LANES : (g + 1) * LANES] = part.astype(jnp.bfloat16)
    member = jnp.where(iota((cells, slots), 0) == keys, 1.0, 0.0)
    mem_ref[:cells, :] = member.astype(jnp.bfloat16)
    block = iota((kc, slots), 0) >> log2(kc // groups)
    block = sum(((block >> b) & 1) << (log2(groups) - 1 - b) for b in range(log2(groups)))
    owned = ((block ^ lax.axis_index("grp")) << log2(kc // groups)) + (iota((kc, slots), 0) & (kc // groups - 1))
    member = jnp.where(owned == (keys >> log2(fg)), 1.0, 0.0)
    mem_ref[cells:, :] = member.astype(jnp.bfloat16)
    ones = jnp.ones((slots, LANES), jnp.bfloat16)
    counts = jnp.dot(mem_ref[...], ones, preferred_element_type=jnp.float32)
    keep_ref[:, width:] = counts[cells : cells + kc // 2]
    send_ref[:, width:] = counts[cells + kc // 2 :]
    share_ref[...] = 1.0 / (1.0 + counts[:cells])
    step = 2 * LANES
    for n in range(width // step):
        at = slice(n * step, (n + 1) * step)
        sums = jnp.dot(mem_ref[...], x_ref[:, at], preferred_element_type=jnp.float32)
        for h in range(2):
            part = slice((2 * n + h) * LANES, (2 * n + h + 1) * LANES)
            new = (old_ref[:, part] + sums[:cells, h * LANES : (h + 1) * LANES]) * share_ref[...]
            new_ref[:, part] = new
            tall_ref[pl.ds(2 * n + h, cells, stride=lane_groups), :] = new
        keep_ref[:, at] = sums[cells : cells + kc // 2]
        send_ref[:, at] = sums[cells + kc // 2 :]
    out_copy = pltpu.make_async_copy(new_ref, out_hbm, sems.at[1])
    out_copy.start()
    key_copy.wait()

    for i in range(steps):
        base = i * (unroll * per_msg)
        for s in range(SLOTS):
            for v in range(0, unroll, 8):
                gaps = []
                for u in range(v, v + 8):
                    at = pl.multiple_of(key_smem[i, u * SLOTS + s], 8)
                    row = wide_ref[pl.ds(base + u * per_msg + s * lane_groups, lane_groups), :]
                    gap = row - tall_ref[pl.ds(at, lane_groups), :]
                    gaps.append(gap * gap)
                gap_ref[pl.ds(s * dests + i * unroll + v, 8), :] = fold(gaps)

    for s in range(SLOTS):
        total = jnp.sum(gap_ref[s * dests : (s + 1) * dests, :], axis=1, keepdims=True)
        dist_ref[:, s : s + 1] = total * (1.0 / width)
    out_copy.wait()


def finish_kernel(back_ref, pos_ref, out_ref, *, dests):
    pos = pos_ref[...]
    dest, rank = pos & (dests - 1), pos >> log2(dests)
    value = back_ref[:, :1]
    for s in range(1, SLOTS):
        value = jnp.where(rank == s, back_ref[:, s : s + 1], value)
    hit = iota((dests, pos.shape[1]), 0) == dest
    out_ref[...] = jnp.sum(jnp.where(hit, value, 0.0), axis=0, keepdims=True)


def call(kernel, outs, scratch=(), limit=24 << 20, **specs):
    return pl.pallas_call(
        kernel,
        out_shape=outs,
        **specs,
        scratch_shapes=list(scratch),
        compiler_params=pltpu.CompilerParams(vmem_limit_bytes=limit),
    )


def pack(coarse_ids, fine_ids, embeddings, dests, groups, kc, fg):
    rows, width = embeddings.shape
    per_msg = SLOTS * (width // LANES) + 2
    f32, bf16, shape = jnp.float32, jnp.bfloat16, jax.ShapeDtypeStruct
    ids = coarse_ids.reshape(1, rows), fine_ids.reshape(1, rows)
    return call(
        functools.partial(pack_kernel, dests=dests, groups=groups, kc=kc, fg=fg),
        (shape((dests * per_msg, LANES), bf16), shape((1, rows), jnp.int32)),
        (
            pltpu.VMEM((1, rows), jnp.int32),
            pltpu.VMEM((1, rows), jnp.int32),
            pltpu.VMEM((rows, width), bf16),
            pltpu.SemaphoreType.DMA((3,)),
            pltpu.VMEM((SLOTS * dests, rows), bf16),
            pltpu.VMEM((dests * per_msg, LANES), f32),
        ),
        in_specs=[pl.BlockSpec(memory_space=pltpu.HBM)] * 3,
    )(*(pltpu.with_memory_space_constraint(a, pltpu.HBM) for a in (ids[0], ids[1], embeddings)))


def update(msg, old, dests, groups, kc, fg):
    cells, width = old.shape
    slots, per_msg = SLOTS * dests, SLOTS * (width // LANES) + 2
    f32, bf16, shape = jnp.float32, jnp.bfloat16, jax.ShapeDtypeStruct
    return call(
        functools.partial(update_kernel, dests=dests, groups=groups, kc=kc, fg=fg),
        (
            shape((kc // 2, width + LANES), f32),
            shape((kc // 2, width + LANES), f32),
            shape((dests, SLOTS), f32),
            shape((cells, width), f32),
        ),
        (
            pltpu.VMEM((dests * per_msg, LANES), f32),
            pltpu.VMEM((slots, width), bf16),
            pltpu.VMEM((cells + kc, slots), bf16),
            pltpu.VMEM((cells, width), f32),
            pltpu.VMEM((cells * width // LANES, LANES), f32),
            pltpu.VMEM((cells, LANES), f32),
            pltpu.VMEM((dests, LANES), jnp.int32),
            pltpu.VMEM((dests // 16, LANES), jnp.int32),
            pltpu.SMEM((dests // 16, LANES), jnp.int32),
            pltpu.VMEM((slots, LANES), f32),
            pltpu.SemaphoreType.DMA((2,)),
        ),
        32 << 20,
        out_specs=(pl.BlockSpec(memory_space=pltpu.VMEM),) * 3 + (pl.BlockSpec(memory_space=pltpu.HBM),),
    )(msg, old)


def finish(back, pos, dests):
    return call(functools.partial(finish_kernel, dests=dests), jax.ShapeDtypeStruct(pos.shape, jnp.float32))(back, pos)


def on_device(embeddings, coarse_ids, fine_ids, coarse_old, fine_old):
    groups = lax.axis_size("grp")
    dests = lax.axis_size("rows") * groups
    rows, width = embeddings.shape
    kc, fg = fine_old.shape[:2]
    cells = kc * fg
    per_msg = SLOTS * (width // LANES) + 2
    msg, pos = pack(coarse_ids, fine_ids, embeddings, dests, groups, kc, fg)
    msg = lax.all_to_all(msg.reshape(dests, per_msg // 2, 2, LANES), AXES, 0, 0, tiled=True)
    coarse, away, dist, new = update(msg.reshape(-1, LANES), fine_old.reshape(cells, width), dests, groups, kc, fg)
    back = lax.all_to_all(dist, AXES, 0, 0, tiled=True)
    rounds = log2(groups)
    coarse = coarse + lax.ppermute(away, "grp", [(g, g ^ 1) for g in range(groups)])
    owned = kc // groups
    parts = [coarse[:owned]]
    for p in range(1, groups // 2):
        partner = sum(((p >> b) & 1) << (rounds - 1 - b) for b in range(rounds))
        parts.append(lax.ppermute(coarse[p * owned : (p + 1) * owned], "grp", [(g, g ^ partner) for g in range(groups)]))
    coarse = functools.reduce(jnp.add, parts)
    coarse_new = (coarse_old + coarse[:, :width]) / (1.0 + coarse[:, width : width + 1])
    distances = finish(back, pos, dests)
    return (coarse_new, new.reshape(fine_old.shape), distances.reshape(rows))


def solution(mesh):
    return jax.shard_map(
        on_device,
        mesh=mesh,
        in_specs=(
            P(AXES, None),
            P(AXES),
            P(AXES),
            P(AXES, None),
            P("rows", "grp", None),
        ),
        out_specs=(P(AXES, None), P("rows", "grp", None), P(AXES)),
        check_vma=False,
    )
```

```python
import functools

import jax
import jax.numpy as jnp
from jax import lax
from jax.experimental import pallas as pl
from jax.experimental.pallas import tpu as pltpu
from jax.sharding import PartitionSpec as P


AXES = ("rows", "grp")
SLOTS = 4
LANES = 128


def log2(n):
    assert n & (n - 1) == 0
    return n.bit_length() - 1


def iota(shape, dim):
    return lax.broadcasted_iota(jnp.int32, shape, dim)


def pack_kernel(
    coarse_hbm,
    fine_hbm,
    emb_hbm,
    msg_ref,
    pos_ref,
    coarse_ref,
    fine_ref,
    emb_ref,
    sems,
    hot_ref,
    wide_ref,
    *,
    dests,
    groups,
    kc,
    fg,
):
    coarse_copy = pltpu.make_async_copy(coarse_hbm, coarse_ref, sems.at[0])
    fine_copy = pltpu.make_async_copy(fine_hbm, fine_ref, sems.at[1])
    emb_copy = pltpu.make_async_copy(emb_hbm, emb_ref, sems.at[2])
    coarse_copy.start()
    fine_copy.start()
    emb_copy.start()
    rows, width = emb_ref.shape
    lane_groups = width // LANES
    per_msg = SLOTS * lane_groups + 2
    coarse_copy.wait()
    fine_copy.wait()
    coarse, fine = coarse_ref[...], fine_ref[...]
    dest = (coarse >> log2(kc)) * groups + (fine >> log2(fg))
    down = jnp.transpose(jnp.broadcast_to(dest, (LANES, rows)))
    ranks = []
    for j in range(0, rows, LANES):
        same = down[: j + LANES] == dest[:, j : j + LANES]
        same = same & (iota((j + LANES, LANES), 0) < iota((j + LANES, LANES), 1) + j)
        ranks.append(jnp.sum(jnp.where(same, 1.0, 0.0), axis=0, keepdims=True))
    rank = jnp.concatenate(ranks, axis=1).astype(jnp.int32)
    pos = rank * dests + dest
    pos_ref[...] = pos
    half = LANES // 2
    names = jnp.where(iota((LANES, rows), 0) < half, (coarse & (kc - 1)) + 1, fine & (fg - 1))
    names = jnp.transpose(names.astype(jnp.float32)).astype(jnp.bfloat16)
    lane = iota((dests, LANES), 1)
    for s in range(SLOTS):
        hit = iota((dests, rows), 0) + s * dests == pos
        hot_ref[s * dests : (s + 1) * dests, :] = jnp.where(hit, 1.0, 0.0).astype(jnp.bfloat16)
    got = jnp.dot(hot_ref[...], names, preferred_element_type=jnp.float32)
    named = jnp.zeros((dests, LANES), jnp.float32)
    for s in range(SLOTS):
        named = jnp.where(lane & (half - 1) == s, got[s * dests : (s + 1) * dests], named)
    at = SLOTS * lane_groups
    wide_ref[pl.ds(at, dests, stride=per_msg), :] = named - jnp.where(lane < half, 1.0, 0.0)
    wide_ref[pl.ds(at + 1, dests, stride=per_msg), :] = jnp.zeros((dests, LANES), jnp.float32)
    emb_copy.wait()
    step = 2 * LANES
    for n in range(width // step):
        got = jnp.dot(hot_ref[...], emb_ref[:, n * step : (n + 1) * step], preferred_element_type=jnp.float32)
        for h in range(2):
            for s in range(SLOTS):
                wide_ref[pl.ds(s * lane_groups + 2 * n + h, dests, stride=per_msg), :] = got[
                    s * dests : (s + 1) * dests, h * LANES : (h + 1) * LANES
                ]
    msg_ref[...] = wide_ref[...].astype(jnp.bfloat16)


def fold(parts):
    parts = [parts[u ^ 3] for u in range(8)]
    row = iota(parts[0].shape, 0)
    low = row < 4
    parts = [
        jnp.where(low, a, b) + pltpu.roll(jnp.where(low, b, a), 4, 0) for a, b in zip(parts[:4], parts[4:])
    ]
    for k in (2, 1):
        kept = (row & k) != 0
        parts = [
            jnp.where(kept, a, b) + jnp.where(kept, pltpu.roll(a, k, 0), pltpu.roll(b, 8 - k, 0))
            for a, b in zip(parts[:k], parts[k:])
        ]
    return parts[0]


def update_kernel(
    msg_ref,
    old_ref,
    keep_ref,
    send_ref,
    dist_ref,
    out_hbm,
    wide_ref,
    mem_ref,
    new_ref,
    tall_ref,
    share_ref,
    column_ref,
    key_ref,
    key_smem,
    gap_ref,
    sems,
    *,
    dests,
    groups,
    kc,
    fg,
):
    cells, width = old_ref.shape
    lane_groups = width // LANES
    per_msg = SLOTS * lane_groups + 2
    slots = SLOTS * dests
    wide_ref[...] = msg_ref[...].astype(jnp.float32)
    names = wide_ref[pl.ds(SLOTS * lane_groups, dests, stride=per_msg), :]
    key = names * fg + pltpu.roll(names, LANES // 2, 1)
    column_ref[...] = jnp.minimum(jnp.maximum(key.astype(jnp.int32), 0), cells - 1) * lane_groups
    unroll = 16
    steps = dests // unroll
    near = jnp.zeros((steps, LANES), jnp.int32)
    for u in range(unroll):
        part = column_ref[pl.ds(u, steps, stride=unroll), :]
        if u:
            part = pltpu.roll(part, u * SLOTS, 1)
        near = jnp.where(iota((steps, LANES), 1) >> log2(SLOTS) == u, part, near)
    key_ref[...] = near
    key_copy = pltpu.make_async_copy(key_ref, key_smem, sems.at[0])
    key_copy.start()
    across = jnp.transpose(key)[:8].astype(jnp.int32)
    keys = jnp.concatenate([across[s : s + 1, :] for s in range(SLOTS)], axis=1)
    member = jnp.where(iota((cells, slots), 0) == keys, 1.0, 0.0)
    mem_ref[:cells, :] = member.astype(jnp.bfloat16)
    block = iota((kc, slots), 0) >> log2(kc // groups)
    block = sum(((block >> b) & 1) << (log2(groups) - 1 - b) for b in range(log2(groups)))
    owned = ((block ^ lax.axis_index("grp")) << log2(kc // groups)) + (iota((kc, slots), 0) & (kc // groups - 1))
    member = jnp.where(owned == (keys >> log2(fg)), 1.0, 0.0)
    mem_ref[cells:, :] = member.astype(jnp.bfloat16)
    ones = jnp.ones((slots, LANES), jnp.bfloat16)
    counts = jnp.dot(mem_ref[...], ones, preferred_element_type=jnp.float32)
    keep_ref[:, width:] = counts[cells : cells + kc // 2]
    send_ref[:, width:] = counts[cells + kc // 2 :]
    share_ref[...] = 1.0 / (1.0 + counts[:cells])
    step = 2 * LANES
    out_copies = []
    for n in range(width // step):
        at = slice(n * step, (n + 1) * step)
        x = jnp.concatenate(
            [
                jnp.concatenate(
                    [
                        wide_ref[pl.ds(s * lane_groups + 2 * n + h, dests, stride=per_msg), :].astype(jnp.bfloat16)
                        for h in range(2)
                    ],
                    axis=1,
                )
                for s in range(SLOTS)
            ],
            axis=0,
        )
        sums = jnp.dot(mem_ref[...], x, preferred_element_type=jnp.float32)
        for h in range(2):
            part = slice((2 * n + h) * LANES, (2 * n + h + 1) * LANES)
            new = (old_ref[:, part] + sums[:cells, h * LANES : (h + 1) * LANES]) * share_ref[...]
            new_ref[:, part] = new
            tall_ref[pl.ds(2 * n + h, cells, stride=lane_groups), :] = new
        out_copies.append(pltpu.make_async_copy(new_ref.at[:, at], out_hbm.at[:, at], sems.at[1 + n]))
        out_copies[n].start()
        keep_ref[:, at] = sums[cells : cells + kc // 2]
        send_ref[:, at] = sums[cells + kc // 2 :]
    key_copy.wait()

    for i in range(steps):
        base = i * (unroll * per_msg)
        for s in range(SLOTS):
            for v in range(0, unroll, 8):
                gaps = []
                for u in range(v, v + 8):
                    at = pl.multiple_of(key_smem[i, u * SLOTS + s], 8)
                    row = wide_ref[pl.ds(base + u * per_msg + s * lane_groups, lane_groups), :]
                    gap = row - tall_ref[pl.ds(at, lane_groups), :]
                    gaps.append(gap * gap)
                gap_ref[pl.ds(s * dests + i * unroll + v, 8), :] = fold(gaps)

    for s in range(SLOTS):
        total = jnp.sum(gap_ref[s * dests : (s + 1) * dests, :], axis=1, keepdims=True)
        dist_ref[:, s : s + 1] = total * (1.0 / width)
    for copy in out_copies:
        copy.wait()


def finish_kernel(back_ref, pos_ref, out_ref, *, dests):
    pos = pos_ref[...]
    dest, rank = pos & (dests - 1), pos >> log2(dests)
    value = back_ref[:, :1]
    for s in range(1, SLOTS):
        value = jnp.where(rank == s, back_ref[:, s : s + 1], value)
    hit = iota((dests, pos.shape[1]), 0) == dest
    out_ref[...] = jnp.sum(jnp.where(hit, value, 0.0), axis=0, keepdims=True)


def call(kernel, outs, scratch=(), limit=24 << 20, **specs):
    return pl.pallas_call(
        kernel,
        out_shape=outs,
        **specs,
        scratch_shapes=list(scratch),
        compiler_params=pltpu.CompilerParams(vmem_limit_bytes=limit),
    )


def pack(coarse_ids, fine_ids, embeddings, dests, groups, kc, fg):
    rows, width = embeddings.shape
    per_msg = SLOTS * (width // LANES) + 2
    f32, bf16, shape = jnp.float32, jnp.bfloat16, jax.ShapeDtypeStruct
    ids = coarse_ids.reshape(1, rows), fine_ids.reshape(1, rows)
    return call(
        functools.partial(pack_kernel, dests=dests, groups=groups, kc=kc, fg=fg),
        (shape((dests * per_msg, LANES), bf16), shape((1, rows), jnp.int32)),
        (
            pltpu.VMEM((1, rows), jnp.int32),
            pltpu.VMEM((1, rows), jnp.int32),
            pltpu.VMEM((rows, width), bf16),
            pltpu.SemaphoreType.DMA((3,)),
            pltpu.VMEM((SLOTS * dests, rows), bf16),
            pltpu.VMEM((dests * per_msg, LANES), f32),
        ),
        in_specs=[pl.BlockSpec(memory_space=pltpu.HBM)] * 3,
    )(*(pltpu.with_memory_space_constraint(a, pltpu.HBM) for a in (ids[0], ids[1], embeddings)))


def update(msg, old, dests, groups, kc, fg):
    cells, width = old.shape
    slots, per_msg = SLOTS * dests, SLOTS * (width // LANES) + 2
    f32, bf16, shape = jnp.float32, jnp.bfloat16, jax.ShapeDtypeStruct
    return call(
        functools.partial(update_kernel, dests=dests, groups=groups, kc=kc, fg=fg),
        (
            shape((kc // 2, width + LANES), f32),
            shape((kc // 2, width + LANES), f32),
            shape((dests, SLOTS), f32),
            shape((cells, width), f32),
        ),
        (
            pltpu.VMEM((dests * per_msg, LANES), f32),
            pltpu.VMEM((cells + kc, slots), bf16),
            pltpu.VMEM((cells, width), f32),
            pltpu.VMEM((cells * width // LANES, LANES), f32),
            pltpu.VMEM((cells, LANES), f32),
            pltpu.VMEM((dests, LANES), jnp.int32),
            pltpu.VMEM((dests // 16, LANES), jnp.int32),
            pltpu.SMEM((dests // 16, LANES), jnp.int32),
            pltpu.VMEM((slots, LANES), f32),
            pltpu.SemaphoreType.DMA((1 + width // (2 * LANES),)),
        ),
        32 << 20,
        out_specs=(pl.BlockSpec(memory_space=pltpu.VMEM),) * 3 + (pl.BlockSpec(memory_space=pltpu.HBM),),
    )(msg, old)


def finish(back, pos, dests):
    return call(functools.partial(finish_kernel, dests=dests), jax.ShapeDtypeStruct(pos.shape, jnp.float32))(back, pos)


def on_device(embeddings, coarse_ids, fine_ids, coarse_old, fine_old):
    groups = lax.axis_size("grp")
    dests = lax.axis_size("rows") * groups
    rows, width = embeddings.shape
    kc, fg = fine_old.shape[:2]
    cells = kc * fg
    per_msg = SLOTS * (width // LANES) + 2
    msg, pos = pack(coarse_ids, fine_ids, embeddings, dests, groups, kc, fg)
    msg = lax.all_to_all(msg.reshape(dests, per_msg // 2, 2, LANES), AXES, 0, 0, tiled=True)
    coarse, away, dist, new = update(msg.reshape(-1, LANES), fine_old.reshape(cells, width), dests, groups, kc, fg)
    back = lax.all_to_all(dist, AXES, 0, 0, tiled=True)
    rounds = log2(groups)
    coarse = coarse + lax.ppermute(away, "grp", [(g, g ^ 1) for g in range(groups)])
    owned = kc // groups
    parts = [coarse[:owned]]
    for p in range(1, groups // 2):
        partner = sum(((p >> b) & 1) << (rounds - 1 - b) for b in range(rounds))
        parts.append(lax.ppermute(coarse[p * owned : (p + 1) * owned], "grp", [(g, g ^ partner) for g in range(groups)]))
    coarse = functools.reduce(jnp.add, parts)
    coarse_new = (coarse_old + coarse[:, :width]) / (1.0 + coarse[:, width : width + 1])
    distances = finish(back, pos, dests)
    return (coarse_new, new.reshape(fine_old.shape), distances.reshape(rows))


def solution(mesh):
    return jax.shard_map(
        on_device,
        mesh=mesh,
        in_specs=(
            P(AXES, None),
            P(AXES),
            P(AXES),
            P(AXES, None),
            P("rows", "grp", None),
        ),
        out_specs=(P(AXES, None), P("rows", "grp", None), P(AXES)),
        check_vma=False,
    )
```

```python
import functools

import jax
import jax.numpy as jnp
from jax import lax
from jax.experimental import pallas as pl
from jax.experimental.pallas import tpu as pltpu
from jax.sharding import PartitionSpec as P


AXES = ("rows", "grp")
SLOTS = 4
LANES = 128


def log2(n):
    assert n & (n - 1) == 0
    return n.bit_length() - 1


def iota(shape, dim):
    return lax.broadcasted_iota(jnp.int32, shape, dim)


def pack_kernel(
    coarse_hbm,
    fine_hbm,
    emb_hbm,
    msg_ref,
    pos_ref,
    coarse_ref,
    fine_ref,
    emb_ref,
    sems,
    hot_ref,
    wide_ref,
    *,
    dests,
    groups,
    kc,
    fg,
):
    coarse_copy = pltpu.make_async_copy(coarse_hbm, coarse_ref, sems.at[0])
    fine_copy = pltpu.make_async_copy(fine_hbm, fine_ref, sems.at[1])
    emb_copy = pltpu.make_async_copy(emb_hbm, emb_ref, sems.at[2])
    coarse_copy.start()
    fine_copy.start()
    emb_copy.start()
    rows, width = emb_ref.shape
    lane_groups = width // LANES
    per_msg = SLOTS * lane_groups + 2
    coarse_copy.wait()
    fine_copy.wait()
    coarse, fine = coarse_ref[...], fine_ref[...]
    dest = (coarse >> log2(kc)) * groups + (fine >> log2(fg))
    down = jnp.transpose(jnp.broadcast_to(dest, (LANES, rows)))
    ranks = []
    for j in range(0, rows, LANES):
        same = down[: j + LANES] == dest[:, j : j + LANES]
        same = same & (iota((j + LANES, LANES), 0) < iota((j + LANES, LANES), 1) + j)
        ranks.append(jnp.sum(jnp.where(same, 1.0, 0.0), axis=0, keepdims=True))
    rank = jnp.concatenate(ranks, axis=1).astype(jnp.int32)
    pos = rank * dests + dest
    pos_ref[...] = pos
    half = LANES // 2
    names = jnp.where(iota((LANES, rows), 0) < half, (coarse & (kc - 1)) + 1, fine & (fg - 1))
    names = jnp.transpose(names.astype(jnp.float32)).astype(jnp.bfloat16)
    lane = iota((dests, LANES), 1)
    for s in range(SLOTS):
        hit = iota((dests, rows), 0) + s * dests == pos
        hot_ref[s * dests : (s + 1) * dests, :] = jnp.where(hit, 1.0, 0.0).astype(jnp.bfloat16)
    got = jnp.dot(hot_ref[...], names, preferred_element_type=jnp.float32)
    named = jnp.zeros((dests, LANES), jnp.float32)
    for s in range(SLOTS):
        named = jnp.where(lane & (half - 1) == s, got[s * dests : (s + 1) * dests], named)
    at = SLOTS * lane_groups
    wide_ref[pl.ds(at, dests, stride=per_msg), :] = named - jnp.where(lane < half, 1.0, 0.0)
    wide_ref[pl.ds(at + 1, dests, stride=per_msg), :] = jnp.zeros((dests, LANES), jnp.float32)
    emb_copy.wait()
    step = 8 * LANES
    for n in range(width // step):
        got = jnp.dot(hot_ref[...], emb_ref[:, n * step : (n + 1) * step], preferred_element_type=jnp.float32)
        for h in range(8):
            for s in range(SLOTS):
                wide_ref[pl.ds(s * lane_groups + 8 * n + h, dests, stride=per_msg), :] = got[
                    s * dests : (s + 1) * dests, h * LANES : (h + 1) * LANES
                ]
    msg_ref[...] = wide_ref[...].astype(jnp.bfloat16)


def fold(parts):
    parts = [parts[u ^ 3] for u in range(8)]
    row = iota(parts[0].shape, 0)
    low = row < 4
    parts = [
        jnp.where(low, a, b) + pltpu.roll(jnp.where(low, b, a), 4, 0) for a, b in zip(parts[:4], parts[4:])
    ]
    for k in (2, 1):
        kept = (row & k) != 0
        parts = [
            jnp.where(kept, a, b) + jnp.where(kept, pltpu.roll(a, k, 0), pltpu.roll(b, 8 - k, 0))
            for a, b in zip(parts[:k], parts[k:])
        ]
    return parts[0]


def update_kernel(
    msg_ref,
    old_ref,
    keep_ref,
    send_ref,
    dist_ref,
    out_hbm,
    wide_ref,
    mem_ref,
    new_ref,
    tall_ref,
    share_ref,
    column_ref,
    key_ref,
    key_smem,
    gap_ref,
    sems,
    *,
    dests,
    groups,
    kc,
    fg,
):
    cells, width = old_ref.shape
    lane_groups = width // LANES
    per_msg = SLOTS * lane_groups + 2
    slots = SLOTS * dests
    wide_ref[...] = msg_ref[...].astype(jnp.float32)
    names = wide_ref[pl.ds(SLOTS * lane_groups, dests, stride=per_msg), :]
    key = names * fg + pltpu.roll(names, LANES // 2, 1)
    column_ref[...] = jnp.minimum(jnp.maximum(key.astype(jnp.int32), 0), cells - 1) * lane_groups
    unroll = 16
    steps = dests // unroll
    near = jnp.zeros((steps, LANES), jnp.int32)
    for u in range(unroll):
        part = column_ref[pl.ds(u, steps, stride=unroll), :]
        if u:
            part = pltpu.roll(part, u * SLOTS, 1)
        near = jnp.where(iota((steps, LANES), 1) >> log2(SLOTS) == u, part, near)
    key_ref[...] = near
    key_copy = pltpu.make_async_copy(key_ref, key_smem, sems.at[0])
    key_copy.start()
    across = jnp.transpose(key)[:8].astype(jnp.int32)
    keys = jnp.concatenate([across[s : s + 1, :] for s in range(SLOTS)], axis=1)
    member = jnp.where(iota((cells, slots), 0) == keys, 1.0, 0.0)
    mem_ref[:cells, :] = member.astype(jnp.bfloat16)
    block = iota((kc, slots), 0) >> log2(kc // groups)
    block = sum(((block >> b) & 1) << (log2(groups) - 1 - b) for b in range(log2(groups)))
    owned = ((block ^ lax.axis_index("grp")) << log2(kc // groups)) + (iota((kc, slots), 0) & (kc // groups - 1))
    member = jnp.where(owned == (keys >> log2(fg)), 1.0, 0.0)
    mem_ref[cells:, :] = member.astype(jnp.bfloat16)
    ones = jnp.ones((slots, LANES), jnp.bfloat16)
    counts = jnp.dot(mem_ref[...], ones, preferred_element_type=jnp.float32)
    keep_ref[:, width:] = counts[cells : cells + kc // 2]
    send_ref[:, width:] = counts[cells + kc // 2 :]
    share_ref[...] = 1.0 / (1.0 + counts[:cells])
    step = 4 * LANES
    out_copies = []
    for n in range(width // step):
        at = slice(n * step, (n + 1) * step)
        x = jnp.concatenate(
            [
                jnp.concatenate(
                    [
                        wide_ref[pl.ds(s * lane_groups + 4 * n + h, dests, stride=per_msg), :].astype(jnp.bfloat16)
                        for h in range(4)
                    ],
                    axis=1,
                )
                for s in range(SLOTS)
            ],
            axis=0,
        )
        sums = jnp.dot(mem_ref[...], x, preferred_element_type=jnp.float32)
        for h in range(4):
            part = slice((4 * n + h) * LANES, (4 * n + h + 1) * LANES)
            new = (old_ref[:, part] + sums[:cells, h * LANES : (h + 1) * LANES]) * share_ref[...]
            new_ref[:, part] = new
            tall_ref[pl.ds(4 * n + h, cells, stride=lane_groups), :] = new
        out_copies.append(pltpu.make_async_copy(new_ref.at[:, at], out_hbm.at[:, at], sems.at[1 + n]))
        out_copies[n].start()
        keep_ref[:, at] = sums[cells : cells + kc // 2]
        send_ref[:, at] = sums[cells + kc // 2 :]
    key_copy.wait()

    for i in range(steps):
        base = i * (unroll * per_msg)
        for s in range(SLOTS):
            for v in range(0, unroll, 8):
                gaps = []
                for u in range(v, v + 8):
                    at = pl.multiple_of(key_smem[i, u * SLOTS + s], 8)
                    row = wide_ref[pl.ds(base + u * per_msg + s * lane_groups, lane_groups), :]
                    gap = row - tall_ref[pl.ds(at, lane_groups), :]
                    gaps.append(gap * gap)
                gap_ref[pl.ds(s * dests + i * unroll + v, 8), :] = fold(gaps)

    for s in range(SLOTS):
        total = jnp.sum(gap_ref[s * dests : (s + 1) * dests, :], axis=1, keepdims=True)
        dist_ref[:, s : s + 1] = total * (1.0 / width)
    for copy in out_copies:
        copy.wait()


def finish_kernel(back_ref, pos_ref, out_ref, *, dests):
    pos = pos_ref[...]
    dest, rank = pos & (dests - 1), pos >> log2(dests)
    value = back_ref[:, :1]
    for s in range(1, SLOTS):
        value = jnp.where(rank == s, back_ref[:, s : s + 1], value)
    hit = iota((dests, pos.shape[1]), 0) == dest
    out_ref[...] = jnp.sum(jnp.where(hit, value, 0.0), axis=0, keepdims=True)


def call(kernel, outs, scratch=(), limit=24 << 20, **specs):
    return pl.pallas_call(
        kernel,
        out_shape=outs,
        **specs,
        scratch_shapes=list(scratch),
        compiler_params=pltpu.CompilerParams(vmem_limit_bytes=limit),
    )


def pack(coarse_ids, fine_ids, embeddings, dests, groups, kc, fg):
    rows, width = embeddings.shape
    per_msg = SLOTS * (width // LANES) + 2
    f32, bf16, shape = jnp.float32, jnp.bfloat16, jax.ShapeDtypeStruct
    ids = coarse_ids.reshape(1, rows), fine_ids.reshape(1, rows)
    return call(
        functools.partial(pack_kernel, dests=dests, groups=groups, kc=kc, fg=fg),
        (shape((dests * per_msg, LANES), bf16), shape((1, rows), jnp.int32)),
        (
            pltpu.VMEM((1, rows), jnp.int32),
            pltpu.VMEM((1, rows), jnp.int32),
            pltpu.VMEM((rows, width), bf16),
            pltpu.SemaphoreType.DMA((3,)),
            pltpu.VMEM((SLOTS * dests, rows), bf16),
            pltpu.VMEM((dests * per_msg, LANES), f32),
        ),
        in_specs=[pl.BlockSpec(memory_space=pltpu.HBM)] * 3,
    )(*(pltpu.with_memory_space_constraint(a, pltpu.HBM) for a in (ids[0], ids[1], embeddings)))


def update(msg, old, dests, groups, kc, fg):
    cells, width = old.shape
    slots, per_msg = SLOTS * dests, SLOTS * (width // LANES) + 2
    f32, bf16, shape = jnp.float32, jnp.bfloat16, jax.ShapeDtypeStruct
    return call(
        functools.partial(update_kernel, dests=dests, groups=groups, kc=kc, fg=fg),
        (
            shape((kc // 2, width + LANES), f32),
            shape((kc // 2, width + LANES), f32),
            shape((dests, SLOTS), f32),
            shape((cells, width), f32),
        ),
        (
            pltpu.VMEM((dests * per_msg, LANES), f32),
            pltpu.VMEM((cells + kc, slots), bf16),
            pltpu.VMEM((cells, width), f32),
            pltpu.VMEM((cells * width // LANES, LANES), f32),
            pltpu.VMEM((cells, LANES), f32),
            pltpu.VMEM((dests, LANES), jnp.int32),
            pltpu.VMEM((dests // 16, LANES), jnp.int32),
            pltpu.SMEM((dests // 16, LANES), jnp.int32),
            pltpu.VMEM((slots, LANES), f32),
            pltpu.SemaphoreType.DMA((1 + width // (4 * LANES),)),
        ),
        32 << 20,
        out_specs=(pl.BlockSpec(memory_space=pltpu.VMEM),) * 3 + (pl.BlockSpec(memory_space=pltpu.HBM),),
    )(msg, old)


def finish(back, pos, dests):
    return call(functools.partial(finish_kernel, dests=dests), jax.ShapeDtypeStruct(pos.shape, jnp.float32))(back, pos)


def on_device(embeddings, coarse_ids, fine_ids, coarse_old, fine_old):
    groups = lax.axis_size("grp")
    dests = lax.axis_size("rows") * groups
    rows, width = embeddings.shape
    kc, fg = fine_old.shape[:2]
    cells = kc * fg
    per_msg = SLOTS * (width // LANES) + 2
    msg, pos = pack(coarse_ids, fine_ids, embeddings, dests, groups, kc, fg)
    msg = lax.all_to_all(msg.reshape(dests, per_msg // 2, 2, LANES), AXES, 0, 0, tiled=True)
    coarse, away, dist, new = update(msg.reshape(-1, LANES), fine_old.reshape(cells, width), dests, groups, kc, fg)
    back = lax.all_to_all(dist, AXES, 0, 0, tiled=True)
    rounds = log2(groups)
    coarse = coarse + lax.ppermute(away, "grp", [(g, g ^ 1) for g in range(groups)])
    owned = kc // groups
    parts = [coarse[:owned]]
    for p in range(1, groups // 2):
        partner = sum(((p >> b) & 1) << (rounds - 1 - b) for b in range(rounds))
        parts.append(lax.ppermute(coarse[p * owned : (p + 1) * owned], "grp", [(g, g ^ partner) for g in range(groups)]))
    coarse = functools.reduce(jnp.add, parts)
    coarse_new = (coarse_old + coarse[:, :width]) / (1.0 + coarse[:, width : width + 1])
    distances = finish(back, pos, dests)
    return (coarse_new, new.reshape(fine_old.shape), distances.reshape(rows))


def solution(mesh):
    return jax.shard_map(
        on_device,
        mesh=mesh,
        in_specs=(
            P(AXES, None),
            P(AXES),
            P(AXES),
            P(AXES, None),
            P("rows", "grp", None),
        ),
        out_specs=(P(AXES, None), P("rows", "grp", None), P(AXES)),
        check_vma=False,
    )
```
